32 devices in a mesh: seq: 8 (over z, y), tensor: 4 (over x, core).
Axes of the slice: x: 2, y: 2, z: 4, core: 2. Of those that a mesh axis runs over, the one named last changes fastest.
Arguments:
- tokens: bfloat16 [3072, 3584], P(('seq', 'tensor')), may hold values from -6 to 6
- gain: float32 [3584], replicated, may hold values from 8 to 32
- weight_codes: int32 [896, 10240], P('seq', 'tensor'), may hold values from -2147483648 to 2147483647, as said below
- scale_exponents: int32 [112, 2560], P(None, 'tensor'), may hold values from 1835887981 to 1886417008, as said below
Outputs:
- projected: bfloat16 [3072, 10240], P(('seq', 'tensor'))
The draws below stay inside these ranges and needn't reach their ends.
Inputs may be any that keep to these rules, and one draw needn't show every extreme that they name: `weight_codes`: every word holds four code bytes. `scale_exponents`: every byte of every word lies between 109 and 112.
All inputs are finite; a program needn't handle non-finite values.
Results may differ from the reference program's by a relative error of at most 0.0049.
Values may be sent and summed in bfloat16 or wider, within the bound.
A program may use at most 128 MiB of HBM per device.

```python
import math
import jax
import jax.numpy as jnp
from jax import lax

D = 3584
FF = 10240
TOKENS = 3072


def scale_levels(key):
    return jax.random.randint(jax.random.fold_in(key, 7), (D // 32, FF), 109, 113, dtype=jnp.int32)


def draw_scale_exponents(key, part):
    levels = scale_levels(key).reshape(D // 32, FF // 4, 4)
    packed_words = jnp.zeros((D // 32, FF // 4), jnp.int32)
    for offset in range(4):
        packed_words = jnp.bitwise_or(packed_words, jnp.left_shift(levels[:, :, offset], 8 * offset))
    return packed_words


def draw_weight_codes(key, part):
    row_levels = jnp.repeat(scale_levels(key), 32, axis=0)
    subkeys = jax.random.split(jax.random.fold_in(key, 11), 4)
    chooser = jax.random.randint(subkeys[0], (D, FF), 0, 16, dtype=jnp.int32)
    further = jax.random.randint(subkeys[1], (D, FF), 3, 16, dtype=jnp.int32)
    depth_drop = jnp.where(chooser < 7, 0, jnp.where(chooser < 14, 1, jnp.where(chooser == 14, 2, further)))
    exponent = jnp.maximum(124 - row_levels - depth_drop, 0)
    negative_bit = jax.random.randint(subkeys[2], (D, FF), 0, 2, dtype=jnp.int32)
    mantissa = jax.random.randint(subkeys[3], (D, FF), 0, 8, dtype=jnp.int32)
    code_bytes = negative_bit * 128 + exponent * 8 + mantissa
    grouped = code_bytes.reshape(D // 4, 4, FF)
    packed_words = jnp.zeros((D // 4, FF), jnp.int32)
    for offset in range(4):
        packed_words = jnp.bitwise_or(packed_words, jnp.left_shift(grouped[:, offset, :], 8 * offset))
    return packed_words


def steps_of(stream_key, shape, cuts, low, largest):
    loudness = 1.0
    for axis_at, shards_of in cuts:
        heights = jax.random.uniform(jax.random.fold_in(jax.random.fold_in(stream_key, 6), axis_at), (shards_of,), jnp.float32, low / len(cuts), largest / len(cuts))
        loudness = loudness * jnp.repeat(jnp.exp(heights), shape[axis_at] // shards_of).reshape((-1,) + (1,) * (len(shape) - 1 - axis_at))
    return loudness


def scatter_about(own_key, dims, width, reach, cuts=(), held_as=jnp.bfloat16):
    values = width * jax.random.normal(own_key, dims, jnp.float32)
    if cuts:
        values = values * steps_of(own_key, dims, cuts, -0.22, 0.18)
    return jnp.clip(values, -reach, reach).astype(held_as)


def setup_inputs(seed: int = 0) -> dict:
    arg_keys = jax.random.split(jax.random.key(seed), 5)
    return {
        "tokens": scatter_about(arg_keys[0], (TOKENS, D), 1.0, 6.0, ((0, 32),)),
        "gain": jnp.clip(jnp.exp(jax.random.uniform(arg_keys[1], (D,), jnp.float32, math.log(8.0), math.log(32.0))), 8.0, 32.0),
        "weight_codes": draw_weight_codes(jax.random.fold_in(arg_keys[4], 71), 0),
        "scale_exponents": draw_scale_exponents(jax.random.fold_in(arg_keys[4], 71), 0),
    }


def decode_values(packed):
    pieces = [jnp.bitwise_and(jnp.right_shift(packed, 8 * offset), 255) for offset in range(4)]
    code_bytes = jnp.stack(pieces, axis=1).reshape(packed.shape[0] * 4, packed.shape[1])
    negative = jnp.right_shift(code_bytes, 7)
    exponent = jnp.bitwise_and(jnp.right_shift(code_bytes, 3), 15)
    mantissa = jnp.bitwise_and(code_bytes, 7).astype(jnp.float32)
    normal = (8.0 + mantissa) * jnp.exp2(exponent.astype(jnp.float32) - 10.0)
    magnitude = jnp.where(exponent == 0, mantissa * 2.0 ** (-9), normal)
    return jnp.where(negative == 1, -magnitude, magnitude)

def decode_scales(packed):
    pieces = [jnp.bitwise_and(jnp.right_shift(packed, 8 * offset), 255) for offset in range(4)]
    scale_bytes = jnp.stack(pieces, axis=2).reshape(packed.shape[0], packed.shape[1] * 4)
    return jnp.exp2(scale_bytes.astype(jnp.float32) - 127.0)

def dequantize(packed, scale_words):
    values = decode_values(packed)
    factors = decode_scales(scale_words)
    groups = scale_words.shape[0]
    columns = packed.shape[1]
    scaled = values.reshape(groups, 32, columns) * factors[:, None, :]
    return scaled.reshape(groups * 32, columns).astype(jnp.bfloat16)

def normalize(tokens, gain):
    wide = tokens.astype(jnp.float32)
    meansq = lax.optimization_barrier(jnp.mean(wide * wide, axis=1, keepdims=True))
    return (wide * lax.rsqrt(meansq + 1e-06) * gain[None, :]).astype(jnp.bfloat16)

def reference(tokens, gain, weight_codes, scale_exponents):
    normed = normalize(tokens, gain)
    block_width = 1024 if FF % 1024 == 0 else FF
    count_blocks = FF // block_width

    def column_block(block_index):
        first_column = block_index * block_width
        code_block = lax.dynamic_slice_in_dim(weight_codes, first_column, block_width, 1)
        scale_block = lax.dynamic_slice_in_dim(scale_exponents, first_column // 4, block_width // 4, 1)
        weight = dequantize(code_block, scale_block)
        return jnp.dot(normed, weight, preferred_element_type=jnp.float32).astype(jnp.bfloat16)
    blocks = lax.map(column_block, jnp.arange(count_blocks, dtype=jnp.int32))
    return jnp.transpose(blocks, (1, 0, 2)).reshape(TOKENS, FF)
```

```python
import functools
import jax
import jax.numpy as jnp
from jax import lax
from jax.experimental import pallas as pl
from jax.experimental.pallas import tpu as pltpu
from jax.sharding import PartitionSpec as P

BOTH = ("seq", "tensor")


def interleave_matrix(words):
    row = lax.broadcasted_iota(jnp.int32, (4 * words, 4 * words), 0)
    col = lax.broadcasted_iota(jnp.int32, (4 * words, 4 * words), 1)
    shift = words.bit_length() - 1
    if words == 1 << shift:
        target = (row & 3) * words + (row >> 2)
        return (target == col).astype(jnp.float32).astype(jnp.bfloat16)
    hit = (row & 3) * words + (row >> 2) == col
    return hit.astype(jnp.float32).astype(jnp.bfloat16)


def word_chunk(words):
    return 128 if words % 128 == 0 else words


def norm_kernel(tokens_ref, gain_ref, out_ref):
    wide = tokens_ref[...].astype(jnp.float32)
    meansq = jnp.mean(wide * wide, axis=1, keepdims=True)
    normed = (wide * lax.rsqrt(meansq + 1e-06) * gain_ref[...]).astype(jnp.bfloat16)
    words = normed.shape[1] // 4
    step = word_chunk(words)
    matrix = interleave_matrix(step)
    for at in range(0, words, step):
        planes = jnp.dot(
            normed[:, 4 * at : 4 * (at + step)], matrix, preferred_element_type=jnp.float32
        ).astype(jnp.bfloat16)
        for k in range(4):
            out_ref[:, k * words + at : k * words + at + step] = planes[:, k * step : (k + 1) * step]


def normalize(tokens, gain):
    return pl.pallas_call(
        norm_kernel,
        out_shape=jax.ShapeDtypeStruct(tokens.shape, jnp.bfloat16),
        cost_estimate=pl.CostEstimate(flops=10**9, bytes_accessed=2 * 2**20, transcendentals=0),
    )(tokens, gain.reshape(1, -1))


def scale_kernel(words_ref, out_ref):
    packed = words_ref[...]
    words = packed.shape[1]
    step = word_chunk(words)
    matrix = interleave_matrix(step)
    planes = []
    for k in range(4):
        level = jnp.bitwise_and(jnp.right_shift(packed, 8 * k), 255) - 109
        planes.append(jnp.left_shift(jnp.ones_like(level), level).astype(jnp.float32).astype(jnp.bfloat16))
    for at in range(0, words, step):
        stacked = jnp.concatenate([p[:, at : at + step] for p in planes], axis=1)
        spread = lax.dot_general(
            stacked, matrix, (((1,), (1,)), ((), ())), preferred_element_type=jnp.float32
        )
        out_ref[:, 4 * at : 4 * (at + step)] = spread * 2.0 ** (-28)


def expand_scales(words):
    return pl.pallas_call(
        scale_kernel,
        out_shape=jax.ShapeDtypeStruct((words.shape[0], 4 * words.shape[1]), jnp.float32),
        cost_estimate=pl.CostEstimate(flops=10**9, bytes_accessed=2 * 2**20, transcendentals=0),
    )(words)


def decode_words(packed, factor, k):
    exponent = jnp.bitwise_and(jnp.right_shift(packed, 8 * k + 3), 15)
    mantissa = jnp.bitwise_and(jnp.right_shift(packed, 8 * k) if k else packed, 7)
    base = jnp.where(exponent > 0, mantissa | 8, mantissa + mantissa)
    value = jnp.left_shift(base, exponent)
    top = jnp.left_shift(packed, 24 - 8 * k) if k < 3 else packed
    value = jnp.where(top < 0, -value, value)
    return value.astype(jnp.float32) * factor


def project_kernel(pieces, order_ref, x_ref, factor_ref, *rest):
    code_refs, out_ref, scratch = rest[:pieces], rest[pieces], rest[pieces + 1 :]
    w_ref = scratch[0]
    rows, columns = code_refs[0].shape
    words = w_ref.shape[0] // 4
    target = scratch[-1]
    align = 16 if rows % 16 == 0 else 8

    @pl.when(pl.program_id(0) == 0)
    def _():
        for piece in range(pieces):
            where = order_ref[piece]
            factor = factor_ref[where]
            packed = code_refs[piece][...].reshape(rows // 8, 8, columns)
            for k in range(4):
                value = decode_words(packed, factor[:, None, :], k).reshape(rows, columns)
                start = pl.multiple_of(k * words + where * rows, align)
                target[pl.ds(start, rows), :] = value.astype(target.dtype)
        if len(scratch) > 1:
            w_ref[...] = target[...].astype(jnp.bfloat16)

    out_ref[...] = jnp.dot(
        x_ref[...], w_ref[...], preferred_element_type=jnp.float32
    ).astype(jnp.bfloat16)


def project(x, factors, codes, order):
    tokens, depth = x.shape
    rows, columns = codes[0].shape
    block = 768 if tokens % 768 == 0 else tokens
    scratch = [pltpu.VMEM((depth, columns), jnp.bfloat16)]
    if rows % 16:
        scratch.append(pltpu.VMEM((depth, columns), jnp.float32))
    whole = lambda shape: pl.BlockSpec(shape, lambda i, o: (0,) * len(shape))
    return pl.pallas_call(
        functools.partial(project_kernel, len(codes)),
        grid_spec=pltpu.PrefetchScalarGridSpec(
            num_scalar_prefetch=1,
            grid=(tokens // block,),
            in_specs=[pl.BlockSpec((block, depth), lambda i, o: (i, 0)), whole(factors.shape)]
            + [whole((rows, columns))] * len(codes),
            out_specs=pl.BlockSpec((block, columns), lambda i, o: (i, 0)),
            scratch_shapes=scratch,
        ),
        out_shape=jax.ShapeDtypeStruct((tokens, columns), jnp.bfloat16),
        compiler_params=pltpu.CompilerParams(vmem_limit_bytes=50 * 2**20),
        cost_estimate=pl.CostEstimate(
            flops=2 * tokens * depth * columns * 2,
            bytes_accessed=2 * tokens * depth + 4 * depth * columns,
            transcendentals=0,
        ),
    )(order, x, factors, *codes)


def place_kernel(widths, parts, order_ref, *refs):
    out_ref = refs[-1]
    total = sum(widths)
    at = 0
    for index in range(parts):
        offset = 0
        for width in widths:
            whole_columns = 128 if total % 128 == 0 else 64
            start = pl.multiple_of(order_ref[index] * total + offset, whole_columns)
            out_ref[:, pl.ds(start, width)] = refs[at][...]
            offset += width
            at += 1


def place(pieces, order, widths):
    rows = pieces[0].shape[0]
    parts = len(pieces) // len(widths)
    total = sum(widths)
    return pl.pallas_call(
        functools.partial(place_kernel, widths, parts),
        grid_spec=pltpu.PrefetchScalarGridSpec(
            num_scalar_prefetch=1,
            grid=(1,),
            in_specs=[pl.BlockSpec(p.shape, lambda i, o: (0, 0)) for p in pieces],
            out_specs=pl.BlockSpec((rows, parts * total), lambda i, o: (0, 0)),
        ),
        out_shape=jax.ShapeDtypeStruct((rows, parts * total), jnp.bfloat16),
        cost_estimate=pl.CostEstimate(flops=0, bytes_accessed=4 * rows * parts * total, transcendentals=0),
    )(order, *pieces)


def chunk_widths(columns):
    if columns % 256 or columns < 1024:
        return (columns,)
    units = columns // 256
    first = (units + 1) // 2
    return (256 * first, 256 * (units - first))


def shards(n_seq, n_tensor, tokens, gain, weight_codes, scale_exponents):
    s = lax.axis_index("seq")
    t = lax.axis_index("tensor")
    half, side = s // 2, s % 2
    rings = n_seq // 2
    columns = weight_codes.shape[1] // 2
    widths = chunk_widths(columns)
    starts = [sum(widths[:j]) for j in range(len(widths))]

    swap = [(i, i ^ 1) for i in range(n_seq)]
    up = [(i, ((i // 2 + 1) % rings) * 2 + i % 2) for i in range(n_seq)]
    down = [(j, i) for i, j in up]

    def cut(which, j):
        return lax.dynamic_slice_in_dim(weight_codes, which * columns + starts[j], widths[j], 1)

    codes = []
    for j in range(len(widths)):
        own = [cut(side, j)]
        other = [lax.ppermute(cut(1 - side, j), "seq", swap)]
        for hop in range(rings - 1):
            own.append(lax.ppermute(own[-1], "seq", up))
            other.append(lax.ppermute(other[-1], "seq", down))
        codes.append(own + other)
    hops = jnp.arange(rings, dtype=jnp.int32)
    order = jnp.concatenate(
        [((half - hops + rings) % rings) * 2 + side, ((half + hops) % rings) * 2 + 1 - side]
    ).astype(jnp.int32)

    x = normalize(tokens, gain)
    masks = []
    x = jnp.concatenate([x, lax.ppermute(x, "seq", swap)], axis=0)
    sources = [(0, 0), (1, 0)]
    bit = n_tensor // 2
    while bit:
        arrived = lax.ppermute(x, "tensor", [(i, i ^ bit) for i in range(n_tensor)])
        x = jnp.concatenate([x, arrived], axis=0)
        sources = sources + [(a, b ^ bit) for a, b in sources]
        bit //= 2

    factors = expand_scales(scale_exponents)
    factors = lax.dynamic_slice_in_dim(factors, side * columns, columns, 1)
    factors = factors.reshape(n_seq, factors.shape[0] // n_seq, columns)

    rows = tokens.shape[0]
    received = [[None] * len(widths) for _ in sources]
    for j, width in enumerate(widths):
        result = project(x, factors[:, :, starts[j] : starts[j] + width], codes[j], order)
        for index, (a, b) in enumerate(sources):
            block = result[index * rows : (index + 1) * rows]
            if a or b:
                perm = [
                    (i * n_tensor + q, (i ^ a) * n_tensor + (q ^ b))
                    for i in range(n_seq)
                    for q in range(n_tensor)
                ]
                block = lax.ppermute(block, BOTH, perm)
            received[index][j] = block
    slots = jnp.stack([(t ^ b) * 2 + (side ^ a) for a, b in sources]).astype(jnp.int32)
    flat = [block for group in received for block in group]
    if columns % 128:
        stacked = jnp.stack([jnp.concatenate(group, axis=1) for group in received])
        ranked = jnp.take(stacked, jnp.argsort(slots), axis=0)
        return jnp.transpose(ranked, (1, 0, 2)).reshape(rows, -1)
    return place(flat, slots, widths)


def solution(mesh):
    body = functools.partial(shards, mesh.shape["seq"], mesh.shape["tensor"])
    return jax.shard_map(
        body,
        mesh=mesh,
        in_specs=(P(BOTH, None), P(), P("seq", "tensor"), P(None, "tensor")),
        out_specs=P(BOTH, None),
        check_vma=False,
    )
```

```python
import functools
import jax
import jax.numpy as jnp
from jax import lax
from jax.experimental import pallas as pl
from jax.experimental.pallas import tpu as pltpu
from jax.sharding import PartitionSpec as P

BOTH = ("seq", "tensor")


def interleave_matrix(words):
    row = lax.broadcasted_iota(jnp.int32, (4 * words, 4 * words), 0)
    col = lax.broadcasted_iota(jnp.int32, (4 * words, 4 * words), 1)
    shift = words.bit_length() - 1
    if words == 1 << shift:
        target = (row & 3) * words + (row >> 2)
        return (target == col).astype(jnp.float32).astype(jnp.bfloat16)
    hit = (row & 3) * words + (row >> 2) == col
    return hit.astype(jnp.float32).astype(jnp.bfloat16)


def word_chunk(words):
    return 128 if words % 128 == 0 else words


def norm_kernel(tokens_ref, gain_ref, out_ref):
    wide = tokens_ref[...].astype(jnp.float32)
    meansq = jnp.mean(wide * wide, axis=1, keepdims=True)
    normed = (wide * lax.rsqrt(meansq + 1e-06) * gain_ref[...]).astype(jnp.bfloat16)
    depth = out_ref.shape[2]
    matrix = interleave_matrix(depth // 4)
    for block in range(out_ref.shape[0]):
        out_ref[block] = jnp.dot(
            normed[:, depth * block : depth * (block + 1)], matrix, preferred_element_type=jnp.float32
        ).astype(jnp.bfloat16)


def normalize(tokens, gain, blocks):
    rows, depth = tokens.shape
    return pl.pallas_call(
        norm_kernel,
        out_shape=jax.ShapeDtypeStruct((blocks, rows, depth // blocks), jnp.bfloat16),
        cost_estimate=pl.CostEstimate(flops=10**9, bytes_accessed=2 * 2**20, transcendentals=0),
    )(tokens, gain.reshape(1, -1))


def scale_kernel(words_ref, out_ref):
    packed = words_ref[...]
    words = packed.shape[1]
    step = word_chunk(words)
    matrix = interleave_matrix(step)
    planes = []
    for k in range(4):
        level = jnp.bitwise_and(jnp.right_shift(packed, 8 * k), 255) - 109
        planes.append(jnp.left_shift(jnp.ones_like(level), level).astype(jnp.float32).astype(jnp.bfloat16))
    for at in range(0, words, step):
        stacked = jnp.concatenate([p[:, at : at + step] for p in planes], axis=1)
        spread = lax.dot_general(
            stacked, matrix, (((1,), (1,)), ((), ())), preferred_element_type=jnp.float32
        )
        out_ref[:, 4 * at : 4 * (at + step)] = spread * 2.0 ** (-28)


def expand_scales(words):
    return pl.pallas_call(
        scale_kernel,
        out_shape=jax.ShapeDtypeStruct((words.shape[0], 4 * words.shape[1]), jnp.float32),
        cost_estimate=pl.CostEstimate(flops=10**9, bytes_accessed=2 * 2**20, transcendentals=0),
    )(words)


def decode_words(packed, factor, k):
    exponent = jnp.bitwise_and(jnp.right_shift(packed, 8 * k + 3), 15)
    mantissa = jnp.bitwise_and(jnp.right_shift(packed, 8 * k) if k else packed, 7)
    base = jnp.where(exponent > 0, mantissa | 8, mantissa + mantissa)
    value = jnp.left_shift(base, exponent)
    top = jnp.left_shift(packed, 24 - 8 * k) if k < 3 else packed
    value = jnp.where(top < 0, -value, value)
    return value.astype(jnp.float32) * factor


def project_kernel(hops, summed, split, order_ref, *refs):
    x_refs, factor_refs = refs[:hops], refs[hops : 2 * hops]
    code_refs = refs[2 * hops : 4 * hops]
    sum_ref = refs[4 * hops] if summed else None
    outs = refs[4 * hops + summed :]
    out_refs, scratch = outs[:split], outs[split:]
    w_ref = scratch[0]
    target = scratch[-1]
    rows, columns = code_refs[0].shape
    align = 16 if rows % 16 == 0 else 8
    side = order_ref[hops]

    @pl.when(pl.program_id(0) == 0)
    def _():
        for hop in range(hops):
            for other in range(2):
                which = 1 - side if other else side
                factor = factor_refs[hop][which][:, None, :]
                packed = code_refs[2 * hop + other][...].reshape(rows // 8, 8, columns)
                for k in range(4):
                    value = decode_words(packed, factor, k).reshape(rows, columns)
                    start = pl.multiple_of((2 * k + which) * rows, align)
                    target[hop, pl.ds(start, rows), :] = value.astype(target.dtype)
        if len(scratch) > 1:
            w_ref[...] = target[...].astype(jnp.bfloat16)

    total = sum_ref[...] if summed else None
    for hop in range(hops):
        part = jnp.dot(x_refs[hop][...], w_ref[hop], preferred_element_type=jnp.float32)
        total = part if total is None else total + part
    height = total.shape[0] // len(out_refs)
    for index, out_ref in enumerate(out_refs):
        out_ref[...] = total[index * height : (index + 1) * height].astype(out_ref.dtype)


def project(x, factors, codes, order, total=None, pieces=1, last=False):
    _, tokens, depth = x.shape
    hops = len(codes) // 2
    rows, columns = codes[0].shape
    block = 768 if tokens % 768 == 0 else tokens
    split = pieces if last and tokens == block else 1
    scratch = [pltpu.VMEM((hops, depth, columns), jnp.bfloat16)]
    if rows % 16:
        scratch.append(pltpu.VMEM((hops, depth, columns), jnp.float32))
    in_specs = [pl.BlockSpec((None, block, depth), lambda i, o, h=h: (o[h], i, 0)) for h in range(hops)]
    in_specs += [
        pl.BlockSpec((None,) + factors.shape[1:], lambda i, o, h=h: (o[h], 0, 0, 0)) for h in range(hops)
    ]
    in_specs += [pl.BlockSpec((rows, columns), lambda i, o: (0, 0))] * len(codes)
    args = [x] * hops + [factors] * hops + list(codes)
    if total is not None:
        in_specs.append(pl.BlockSpec((block, columns), lambda i, o: (i, 0)))
        args.append(total)
    kind = jnp.bfloat16 if last else jnp.float32
    out = pl.pallas_call(
        functools.partial(project_kernel, hops, int(total is not None), split),
        grid_spec=pltpu.PrefetchScalarGridSpec(
            num_scalar_prefetch=1,
            grid=(tokens // block,),
            in_specs=in_specs,
            out_specs=[pl.BlockSpec((block // split, columns), lambda i, o: (i, 0))] * split,
            scratch_shapes=scratch,
        ),
        out_shape=[jax.ShapeDtypeStruct((tokens // split, columns), kind)] * split,
        compiler_params=pltpu.CompilerParams(vmem_limit_bytes=50 * 2**20),
        cost_estimate=pl.CostEstimate(
            flops=2 * tokens * depth * columns * 2 * hops,
            bytes_accessed=2 * tokens * depth * hops + 4 * depth * columns,
            transcendentals=0,
        ),
    )(order, *args)
    if not last:
        return out[0]
    if split == pieces:
        return out
    height = tokens // pieces
    return [out[0][i * height : (i + 1) * height] for i in range(pieces)]


def place_kernel(widths, parts, order_ref, *refs):
    out_ref = refs[-1]
    total = sum(widths)
    at = 0
    for index in range(parts):
        offset = 0
        for width in widths:
            whole_columns = 128 if total % 128 == 0 else 64
            start = pl.multiple_of(order_ref[index] * total + offset, whole_columns)
            out_ref[:, pl.ds(start, width)] = refs[at][...]
            offset += width
            at += 1


def place(pieces, order, widths):
    rows = pieces[0].shape[0]
    parts = len(pieces) // len(widths)
    total = sum(widths)
    return pl.pallas_call(
        functools.partial(place_kernel, widths, parts),
        grid_spec=pltpu.PrefetchScalarGridSpec(
            num_scalar_prefetch=1,
            grid=(1,),
            in_specs=[pl.BlockSpec(p.shape, lambda i, o: (0, 0)) for p in pieces],
            out_specs=pl.BlockSpec((rows, parts * total), lambda i, o: (0, 0)),
        ),
        out_shape=jax.ShapeDtypeStruct((rows, parts * total), jnp.bfloat16),
        cost_estimate=pl.CostEstimate(flops=0, bytes_accessed=4 * rows * parts * total, transcendentals=0),
    )(order, *pieces)


def chunk_widths(columns):
    if columns % 256 or columns < 1024:
        return (columns,)
    units = columns // 256
    first = (units + 1) // 2
    return (256 * first, 256 * (units - first))


def shards(n_seq, n_tensor, tokens, gain, weight_codes, scale_exponents):
    return layer(n_seq, n_tensor, tokens, gain, weight_codes, scale_exponents)


def layer(n_seq, n_tensor, tokens, gain, weight_codes, scale_exponents):
    s = lax.axis_index("seq")
    t = lax.axis_index("tensor")
    half, side = s // 2, s % 2
    rings = n_seq // 2
    columns = weight_codes.shape[1] // 2
    widths = chunk_widths(columns)
    starts = [sum(widths[:j]) for j in range(len(widths))]

    swap = [(i, i ^ 1) for i in range(n_seq)]
    up = [(i, ((i // 2 + 1) % rings) * 2 + i % 2) for i in range(n_seq)]

    def cut(which, j):
        return lax.dynamic_slice_in_dim(weight_codes, which * columns + starts[j], widths[j], 1)

    codes = []
    for j in range(len(widths)):
        own = [cut(side, j)]
        other = [lax.ppermute(cut(1 - side, j), "seq", swap)]
        for _ in range(1, rings):
            own.append(lax.ppermute(own[-1], "seq", up))
            other.append(lax.ppermute(other[-1], "seq", up))
        codes.append([piece for pair in zip(own, other) for piece in pair])
    order = [(half - hop + rings) % rings for hop in range(rings)]
    early = jnp.stack(order[:-1] + [side]).astype(jnp.int32)
    late = jnp.stack(order[-1:] + [side]).astype(jnp.int32)

    x = normalize(tokens, gain, rings)
    factors = expand_scales(scale_exponents)
    factors = lax.dynamic_slice_in_dim(factors, side * columns, columns, 1)
    factors = factors.reshape(rings, 2, factors.shape[0] // n_seq, columns)
    arrived = lax.ppermute(x, "seq", swap)
    arrived, factors = lax.optimization_barrier((arrived, factors))
    x = jnp.concatenate([x, arrived], axis=1)
    sources = [(0, 0), (1, 0)]
    bit = n_tensor // 2
    while bit:
        arrived = lax.ppermute(x, "tensor", [(i, i ^ bit) for i in range(n_tensor)])
        x = jnp.concatenate([x, arrived], axis=1)
        sources = sources + [(a, b ^ bit) for a, b in sources]
        bit = bit // 2

    rows = tokens.shape[0]
    received = [[None] * len(widths) for _ in sources]
    for j, width in enumerate(widths):
        scale = factors[:, :, :, starts[j] : starts[j] + width]
        total = project(x, scale, codes[j][:-2], early)
        blocks = project(x, scale, codes[j][-2:], late, total, len(sources), True)
        for index, (a, b) in enumerate(sources):
            block = blocks[index]
            if a or b:
                perm = [
                    (i * n_tensor + q, (i ^ a) * n_tensor + (q ^ b))
                    for i in range(n_seq)
                    for q in range(n_tensor)
                ]
                block = lax.ppermute(block, BOTH, perm)
            received[index][j] = block
    slots = jnp.stack([(t ^ b) * 2 + (side ^ a) for a, b in sources]).astype(jnp.int32)
    flat = [block for group in received for block in group]
    if columns % 128:
        stacked = jnp.stack([jnp.concatenate(group, axis=1) for group in received])
        ranked = jnp.take(stacked, jnp.argsort(slots), axis=0)
        return jnp.transpose(ranked, (1, 0, 2)).reshape(rows, -1)
    return place(flat, slots, widths)


def solution(mesh):
    n_seq, n_tensor = mesh.shape["seq"], mesh.shape["tensor"]
    return jax.shard_map(
        functools.partial(shards, n_seq, n_tensor),
        mesh=mesh,
        in_specs=(P(BOTH, None), P(), P("seq", "tensor"), P(None, "tensor")),
        out_specs=P(BOTH, None),
        check_vma=False,
    )
```
